128 devices in a mesh: dp: 1, ep: 128 (over z, y, x, core).
Axes of the slice: x: 4, y: 4, z: 4, core: 2. Of those that a mesh axis runs over, the one named last changes fastest.
Arguments:
- x_tok: bfloat16 [49152, 2048], P(('dp', 'ep'))
- topk_idx: int32 [49152, 8], P(('dp', 'ep'))
- topk_w: float32 [49152, 8], P(('dp', 'ep'))
- w_in: bfloat16 [256, 2048, 512], P('ep')
- w_out: bfloat16 [256, 512, 2048], P('ep')
- shared_in: bfloat16 [2048, 512], replicated
- shared_out: bfloat16 [512, 2048], replicated
Outputs:
- output: bfloat16 [49152, 2048], P(('dp', 'ep'))
All inputs are finite; a program needn't handle non-finite values.
Results may differ from the reference program's by a relative error of at most 0.001.
Values are sent between devices in bfloat16 or wider.
A program may use at most 1 GiB of HBM per device.

```python
import jax
import jax.numpy as jnp
from jax import lax

GROUP_SIZE = 128
TOK_DEV = 384
D_MODEL = 2048
FF_DIM = 512
FS_DIM = 512
EXPERTS = 256
TOP_K = 8
NUM_HOT = 8
SLOT_CAP = 36

TOKENS = GROUP_SIZE * TOK_DEV
EXPERT_ROWS = SLOT_CAP * GROUP_SIZE


def draw_routing(route_key):
    key_hot, key_extra, key_tok, key_rot = jax.random.split(route_key, 4)
    cold_count = EXPERTS - NUM_HOT
    rest_pairs = TOK_DEV * TOP_K - NUM_HOT * SLOT_CAP
    base_load = rest_pairs // cold_count
    extra_pairs = rest_pairs - base_load * cold_count
    expert_order = jax.random.permutation(key_hot, EXPERTS)
    cold_rank = jax.vmap(lambda dev_key: jax.random.permutation(dev_key, cold_count))(jax.random.split(key_extra, GROUP_SIZE))
    cold_load = base_load + (cold_rank < extra_pairs).astype(jnp.int32)
    hot_load = jnp.full((GROUP_SIZE, NUM_HOT), SLOT_CAP, jnp.int32)
    ordered_load = jnp.concatenate([hot_load, cold_load], axis=1)
    expert_load = jnp.zeros((GROUP_SIZE, EXPERTS), jnp.int32).at[:, expert_order].set(ordered_load)
    load_ends = jnp.cumsum(expert_load, axis=1)
    pair_ids = jnp.arange(TOK_DEV * TOP_K, dtype=jnp.int32)
    pair_expert = jax.vmap(lambda ends_row: jnp.searchsorted(ends_row, pair_ids, side='right'))(load_ends)
    slot_table = pair_expert.reshape(GROUP_SIZE, TOP_K, TOK_DEV).transpose(0, 2, 1)
    tok_perm = jax.vmap(lambda dev_key: jax.random.permutation(dev_key, TOK_DEV))(jax.random.split(key_tok, GROUP_SIZE))
    tok_index = jnp.broadcast_to(tok_perm[:, :, None], (GROUP_SIZE, TOK_DEV, TOP_K))
    slot_table = jnp.take_along_axis(slot_table, tok_index, axis=1)
    slot_shift = jax.random.randint(key_rot, (GROUP_SIZE, TOK_DEV, 1), 0, TOP_K)
    slot_cols = (jnp.arange(TOP_K)[None, None, :] + slot_shift) % TOP_K
    slot_table = jnp.take_along_axis(slot_table, slot_cols, axis=2)
    return slot_table.reshape(TOKENS, TOP_K).astype(jnp.int32)


def draw_stack(stack_key, fan_in, fan_out):
    def one_expert(expert_key):
        return (jax.random.normal(expert_key, (fan_in, fan_out), jnp.float32) * fan_in ** -0.5).astype(jnp.bfloat16)
    return lax.map(one_expert, jax.random.split(stack_key, EXPERTS))


def setup_inputs(seed: int = 0, part: int = 0) -> dict:
    root_key = jax.random.key(seed)
    key_x, key_route, key_gate, key_in, key_out, key_sin, key_sout = jax.random.split(root_key, 7)
    x_tok = jax.random.normal(jax.random.fold_in(key_x, part), (TOKENS, D_MODEL), jnp.float32).astype(jnp.bfloat16)
    topk_idx = draw_routing(jax.random.fold_in(key_route, part))
    gate_raw = jax.random.uniform(jax.random.fold_in(key_gate, part), (TOKENS, TOP_K), jnp.float32, 0.2, 1.0)
    topk_w = gate_raw * (1.5 / TOP_K ** 0.5)
    w_in = draw_stack(key_in, D_MODEL, FF_DIM)
    w_out = draw_stack(key_out, FF_DIM, D_MODEL)
    shared_in = (jax.random.normal(key_sin, (D_MODEL, FS_DIM), jnp.float32) * D_MODEL ** -0.5).astype(jnp.bfloat16)
    shared_out = (jax.random.normal(key_sout, (FS_DIM, D_MODEL), jnp.float32) * FS_DIM ** -0.5).astype(jnp.bfloat16)
    return {'x_tok': x_tok, 'topk_idx': topk_idx, 'topk_w': topk_w, 'w_in': w_in, 'w_out': w_out, 'shared_in': shared_in, 'shared_out': shared_out}


def reference(x_tok, topk_idx, topk_w, w_in, w_out, shared_in, shared_out):
    pair_total = TOKENS * TOP_K
    flat_ids = topk_idx.reshape(pair_total)
    pair_order = jnp.argsort(flat_ids, stable=True)
    counts = jnp.zeros((EXPERTS,), jnp.int32).at[flat_ids].add(1)
    starts = jnp.cumsum(counts) - counts
    pair_gates = topk_w.astype(jnp.bfloat16).astype(jnp.float32).reshape(pair_total)
    slot_ids = jnp.arange(EXPERT_ROWS)

    def expert_step(routed_acc, step_in):
        e_index, w_first, w_second = step_in
        slot_valid = slot_ids < counts[e_index]
        pair_pos = pair_order[jnp.minimum(starts[e_index] + slot_ids, pair_total - 1)]
        tok_pos = pair_pos // TOP_K
        gathered = x_tok[tok_pos]
        hidden = jax.nn.gelu(jnp.dot(gathered, w_first, preferred_element_type=jnp.float32), approximate=True).astype(jnp.bfloat16)
        expert_out = jnp.dot(hidden, w_second, preferred_element_type=jnp.float32).astype(jnp.bfloat16)
        pair_scale = jnp.where(slot_valid, pair_gates[pair_pos], 0.0)
        contrib = expert_out.astype(jnp.float32) * pair_scale[:, None]
        return routed_acc.at[tok_pos].add(contrib), None

    routed_init = jnp.zeros((TOKENS, D_MODEL), jnp.float32)
    routed, _ = lax.scan(expert_step, routed_init, (jnp.arange(EXPERTS), w_in, w_out))
    shared_hidden = jax.nn.gelu(jnp.dot(x_tok, shared_in, preferred_element_type=jnp.float32), approximate=True).astype(jnp.bfloat16)
    shared_val = jnp.dot(shared_hidden, shared_out, preferred_element_type=jnp.float32)
    return (routed + shared_val).astype(jnp.bfloat16)
```

```python
import jax
import jax.numpy as jnp
from jax import lax
from jax.sharding import PartitionSpec as P

LOAD_MULT = 3
BASE_CAP = 12
HOT = 8
TILE = 8
BF16 = jnp.bfloat16
F32 = jnp.float32


def gelu(z):
    return jax.nn.gelu(z, approximate=True)


def slot_tables(topk_idx, topk_w, num_experts, slot_cap):
    tok_rows, top_k = topk_idx.shape
    expert_hot = (topk_idx[:, :, None] == jnp.arange(num_experts, dtype=jnp.int32)).astype(jnp.int32)
    running = jnp.cumsum(expert_hot.reshape(tok_rows * top_k, num_experts), axis=0)
    slot_pos = jnp.sum(running.reshape(tok_rows, top_k, num_experts) * expert_hot, axis=2) - 1
    slot_hot = (slot_pos[:, :, None] == jnp.arange(slot_cap, dtype=jnp.int32)).astype(BF16)
    gate_hot = expert_hot.astype(BF16) * topk_w.astype(BF16)[:, :, None]
    combine = jnp.einsum('tje,tjc->tec', gate_hot, slot_hot, preferred_element_type=F32).astype(BF16)
    dispatch = (combine != 0).astype(BF16)
    return combine, dispatch


def solution(mesh):
    group_size = mesh.shape['ep']
    members = group_size // HOT
    hot_teams = [[h * members + r for r in range(members)] for h in range(HOT)]
    hot_lanes = [[h * members + r for h in range(HOT)] for r in range(members)]

    def wide_layer(x_loc, idx_loc, gate_loc, w_in, w_out, shared_val):
        tok_rows, top_k = idx_loc.shape
        num_experts = w_in.shape[0] * group_size
        slot_cap = min(tok_rows, LOAD_MULT * tok_rows * top_k // num_experts)
        combine, dispatch = slot_tables(idx_loc, gate_loc, num_experts, slot_cap)
        send_rows = jnp.einsum('tec,tm->ecm', dispatch, x_loc, preferred_element_type=F32).astype(BF16)
        recv_rows = lax.all_to_all(send_rows, 'ep', 0, 1, tiled=True)
        hidden = gelu(jnp.einsum('erm,emf->erf', recv_rows, w_in, preferred_element_type=F32)).astype(BF16)
        expert_out = jnp.einsum('erf,efm->erm', hidden, w_out, preferred_element_type=F32).astype(BF16)
        back_rows = lax.all_to_all(expert_out, 'ep', 1, 0, tiled=True)
        routed = jnp.einsum('tec,ecm->tm', combine, back_rows, preferred_element_type=F32)
        return (routed + shared_val).astype(BF16)

    def local_layer(x_loc, idx_loc, gate_loc, w_in, w_out, shared_in, shared_out):
        tok_rows, top_k = idx_loc.shape
        d_model = x_loc.shape[1]
        per_dev = w_in.shape[0]
        num_experts = per_dev * group_size
        slot_cap = min(tok_rows, LOAD_MULT * tok_rows * top_k // num_experts)
        base_cap = min(BASE_CAP, slot_cap)
        over_cap = slot_cap - base_cap
        me = lax.axis_index('ep')

        expert_ids = jnp.arange(num_experts, dtype=jnp.int32)
        pick = idx_loc[:, :, None] == expert_ids
        picked = jnp.any(pick, axis=1)
        gate_rows = gate_loc.astype(BF16).astype(F32)
        gates = jnp.sum(jnp.where(pick, gate_rows[:, :, None], 0.0), axis=1).astype(BF16)
        ones = picked.astype(BF16)
        before = (jnp.arange(tok_rows)[:, None] > jnp.arange(tok_rows)[None, :]).astype(BF16)
        rank = jnp.dot(before, ones, preferred_element_type=F32)
        slot = jnp.where(picked, rank, -1.0).astype(BF16)

        counts = jnp.sum(picked.astype(jnp.int32), axis=0)
        peak = lax.pmax(counts, 'ep')
        over = peak > base_cap
        over_rank = jnp.cumsum(over.astype(jnp.int32)) - 1
        fits = jnp.sum(over.astype(jnp.int32)) <= HOT
        hot_sel = (over[:, None] & (over_rank[:, None] == jnp.arange(HOT, dtype=jnp.int32))).astype(BF16)

        mine = lax.dynamic_slice(hot_sel, (me * per_dev, 0), (per_dev, HOT))

        def to_team(w):
            rows, cols = w.shape[1:]
            spread = jnp.zeros((HOT, rows, cols), BF16)
            for k in range(per_dev):
                spread = jnp.where((mine[k] != 0)[:, None, None], w[k][None], spread)
            piece = lax.psum_scatter(spread.reshape(HOT * rows, cols), 'ep', scatter_dimension=0, tiled=True)
            return lax.all_gather(piece, 'ep', axis_index_groups=hot_teams, axis=0, tiled=True)

        hot_in = to_team(w_in)
        hot_out = to_team(w_out)

        base_rows = num_experts * base_cap
        owner = jnp.arange(base_rows, dtype=jnp.int32) // base_cap
        place = (jnp.arange(base_rows, dtype=jnp.int32) % base_cap).astype(F32)
        repeat = (expert_ids[:, None] == owner[None, :]).astype(BF16)
        slot_of = jnp.dot(slot, repeat, preferred_element_type=F32)
        gate_of = jnp.dot(gates, repeat, preferred_element_type=F32)
        base_unit = (slot_of == place).astype(BF16)
        base_gate = jnp.where(slot_of == place, gate_of, 0.0).astype(BF16)

        hot_rows = HOT * over_cap
        hot_owner = jnp.arange(hot_rows, dtype=jnp.int32) // over_cap
        hot_place = (jnp.arange(hot_rows, dtype=jnp.int32) % over_cap + base_cap).astype(F32)
        hot_repeat = (jnp.arange(HOT, dtype=jnp.int32)[:, None] == hot_owner[None, :]).astype(BF16)
        hot_map = jnp.dot(hot_sel, hot_repeat, preferred_element_type=F32).astype(BF16)
        hot_slot_of = jnp.dot(slot, hot_map, preferred_element_type=F32)
        hot_gate_of = jnp.dot(gates, hot_map, preferred_element_type=F32)
        hot_unit = (hot_slot_of == hot_place).astype(BF16)
        hot_gate = jnp.where(hot_slot_of == hot_place, hot_gate_of, 0.0).astype(BF16)

        send = jnp.einsum('tr,tm->rm', base_unit, x_loc, preferred_element_type=F32).astype(BF16)
        recv = lax.all_to_all(send.reshape(group_size, per_dev * base_cap, d_model), 'ep', 0, 0, tiled=True)
        hot_send = jnp.einsum('tr,tm->rm', hot_unit, x_loc, preferred_element_type=F32).astype(BF16)
        hot_recv = lax.all_to_all(hot_send.reshape(HOT, over_cap, d_model), 'ep', 0, 0, axis_index_groups=hot_lanes, tiled=True)

        def ffn(rows, first, second):
            hidden = gelu(jnp.dot(rows, first, preferred_element_type=F32)).astype(BF16)
            return jnp.dot(hidden, second, preferred_element_type=F32)

        span = 2 * TILE
        first = ffn(recv[:, :span].reshape(group_size * span, d_model), w_in[0], w_out[0]).astype(BF16)
        second = ffn(recv[:, TILE:].reshape(group_size * span, d_model), w_in[1], w_out[1]).astype(BF16)
        first = first.reshape(group_size, span, d_model)
        second = second.reshape(group_size, span, d_model)
        middle = jnp.where(jnp.arange(TILE)[None, :, None] < base_cap - TILE, first[:, TILE:], second[:, :TILE])
        done = jnp.concatenate([first[:, :TILE], middle, second[:, TILE:]], axis=1)
        hot_done = ffn(hot_recv.reshape(hot_rows, d_model), hot_in, hot_out).astype(BF16)

        back = lax.all_to_all(done, 'ep', 0, 0, tiled=True).reshape(base_rows, d_model)
        hot_back = lax.all_to_all(hot_done.reshape(HOT, over_cap, d_model), 'ep', 0, 0, axis_index_groups=hot_lanes, tiled=True)
        hot_back = hot_back.reshape(hot_rows, d_model)

        shared_val = ffn(x_loc, shared_in, shared_out)
        routed = jnp.dot(base_gate, back, preferred_element_type=F32) + jnp.dot(hot_gate, hot_back, preferred_element_type=F32)
        tight = (routed + shared_val).astype(BF16)
        return lax.cond(
            fits,
            lambda *_: tight,
            lambda *args: wide_layer(*args),
            x_loc, idx_loc, gate_loc, w_in, w_out, shared_val,
        )

    tok_spec = P(('dp', 'ep'), None)
    expert_spec = P('ep', None, None)
    whole_spec = P(None, None)
    return jax.shard_map(local_layer, mesh=mesh, in_specs=(tok_spec, tok_spec, tok_spec, expert_spec, expert_spec, whole_spec, whole_spec), out_specs=tok_spec, check_vma=False)
```

```python
import functools

import jax
import jax.numpy as jnp
from jax import lax
from jax.experimental import pallas as pl
from jax.experimental.pallas import tpu as pltpu
from jax.sharding import PartitionSpec as P

LOAD_MULT = 3
BASE_CAP = 12
HOT = 8
CORES = 2
TILE = 8
STRIDE = 37
BF16 = jnp.bfloat16
F32 = jnp.float32
MESH = pl.DeviceIdType.MESH


def gelu(z):
    return jax.nn.gelu(z, approximate=True)


def slot_tables(topk_idx, topk_w, num_experts, slot_cap):
    tok_rows, top_k = topk_idx.shape
    expert_hot = (topk_idx[:, :, None] == jnp.arange(num_experts, dtype=jnp.int32)).astype(jnp.int32)
    running = jnp.cumsum(expert_hot.reshape(tok_rows * top_k, num_experts), axis=0)
    slot_pos = jnp.sum(running.reshape(tok_rows, top_k, num_experts) * expert_hot, axis=2) - 1
    slot_hot = (slot_pos[:, :, None] == jnp.arange(slot_cap, dtype=jnp.int32)).astype(BF16)
    gate_hot = expert_hot.astype(BF16) * topk_w.astype(BF16)[:, :, None]
    combine = jnp.einsum('tje,tjc->tec', gate_hot, slot_hot, preferred_element_type=F32).astype(BF16)
    dispatch = (combine != 0).astype(BF16)
    return combine, dispatch


def send_to(src, dst, send_sem, recv_sem, peer):
    return pltpu.make_async_remote_copy(
        src_ref=src, dst_ref=dst, send_sem=send_sem, recv_sem=recv_sem,
        device_id={'ep': peer}, device_id_type=MESH,
    )


def peer_of(me, step, n):
    return lax.rem(me + step * STRIDE, n)


def wait_bytes(like_src, like_dst, sem):
    pltpu.make_async_copy(like_src, like_dst, sem).wait()


def counts_kernel(n, mine, peak, table, send_sem, recv_sem, own_sem):
    me = lax.axis_index('ep')
    own = pltpu.make_async_copy(mine, table.at[me], own_sem)
    own.start()

    def start(step, carry):
        send_to(mine, table.at[me], send_sem, recv_sem, peer_of(me, step, n)).start()
        return carry

    lax.fori_loop(1, n, start, 0)
    own.wait()
    wait_bytes(table.at[pl.ds(0, n - 1)], table.at[pl.ds(0, n - 1)], recv_sem)
    wait_bytes(table.at[pl.ds(0, n - 1)], table.at[pl.ds(0, n - 1)], send_sem)
    peak[...] = jnp.max(table[...], axis=0)


def hot_rows_out(me, hot, members, src, dst, send_sem, recv_sem, own_sem):
    team, lane = me // members, lax.rem(me, members)
    pltpu.make_async_copy(src.at[team], dst.at[team], own_sem).start()
    for step in range(1, hot):
        other = lax.rem(team + step, hot)
        send_to(src.at[other], dst.at[team], send_sem, recv_sem, other * members + lane).start()


def hot_rows_wait(hot, src, dst, send_sem, recv_sem, own_sem):
    wait_bytes(src.at[0], dst.at[0], own_sem)
    wait_bytes(src.at[pl.ds(0, hot - 1)], dst.at[pl.ds(0, hot - 1)], recv_sem)
    wait_bytes(src.at[pl.ds(0, hot - 1)], dst.at[pl.ds(0, hot - 1)], send_sem)


def dispatch_kernel(
    n, hot, source, rows, hot_rows, slices, recv, hot_recv, team_w,
    landed, chosen, base_sems, hot_sems, slice_sems, team_sems,
):
    me = lax.axis_index('ep')
    members = n // hot

    def scatter(step, carry):
        peer = peer_of(me, step, n)
        send_to(slices.at[peer], landed.at[me], slice_sems.at[0], slice_sems.at[1], peer).start()
        return carry

    def base(step, carry):
        peer = peer_of(me, step, n)
        send_to(rows.at[peer], recv.at[me], base_sems.at[0], base_sems.at[1], peer).start()
        return carry

    def spread(step, carry):
        peer = peer_of(me, step, n)
        send_to(chosen.at[peer // members], team_w.at[me], team_sems.at[0], team_sems.at[1], peer).start()
        return carry

    lax.fori_loop(1, n, scatter, 0)
    pltpu.make_async_copy(slices.at[me], landed.at[me], slice_sems.at[2]).start()
    hot_rows_out(me, hot, members, hot_rows, hot_recv, hot_sems.at[0], hot_sems.at[1], hot_sems.at[2])
    pltpu.make_async_copy(rows.at[me], recv.at[me], base_sems.at[2]).start()
    half = n // 2
    lax.fori_loop(1, half, base, 0)

    wait_bytes(slices.at[0], landed.at[0], slice_sems.at[2])
    wait_bytes(slices.at[pl.ds(0, n - 1)], landed.at[pl.ds(0, n - 1)], slice_sems.at[1])
    for h in range(hot):
        chosen[h] = landed[source[h]]
    lax.fori_loop(half, n, base, 0)
    pltpu.make_async_copy(chosen.at[me // members], team_w.at[me], team_sems.at[2]).start()
    lax.fori_loop(1, n, spread, 0)

    wait_bytes(slices.at[pl.ds(0, n - 1)], landed.at[pl.ds(0, n - 1)], slice_sems.at[0])
    hot_rows_wait(hot, hot_rows, hot_recv, hot_sems.at[0], hot_sems.at[1], hot_sems.at[2])
    wait_bytes(rows.at[0], recv.at[0], base_sems.at[2])
    wait_bytes(rows.at[pl.ds(0, n - 1)], recv.at[pl.ds(0, n - 1)], base_sems.at[1])
    wait_bytes(rows.at[pl.ds(0, n - 1)], recv.at[pl.ds(0, n - 1)], base_sems.at[0])
    wait_bytes(chosen.at[0], team_w.at[0], team_sems.at[2])
    wait_bytes(slices.at[pl.ds(0, n - 1)], team_w.at[pl.ds(0, n - 1)], team_sems.at[1])
    wait_bytes(slices.at[pl.ds(0, n - 1)], team_w.at[pl.ds(0, n - 1)], team_sems.at[0])


def return_kernel(n, hot, rows, hot_rows, recv, hot_recv, base_sems, hot_sems):
    me = lax.axis_index('ep')
    members = n // hot

    def base(step, carry):
        peer = peer_of(me, step, n)
        send_to(rows.at[peer], recv.at[me], base_sems.at[0], base_sems.at[1], peer).start()
        return carry

    hot_rows_out(me, hot, members, hot_rows, hot_recv, hot_sems.at[0], hot_sems.at[1], hot_sems.at[2])
    pltpu.make_async_copy(rows.at[me], recv.at[me], base_sems.at[2]).start()
    lax.fori_loop(1, n, base, 0)
    hot_rows_wait(hot, hot_rows, hot_recv, hot_sems.at[0], hot_sems.at[1], hot_sems.at[2])
    wait_bytes(rows.at[0], recv.at[0], base_sems.at[2])
    wait_bytes(rows.at[pl.ds(0, n - 1)], recv.at[pl.ds(0, n - 1)], base_sems.at[1])
    wait_bytes(rows.at[pl.ds(0, n - 1)], recv.at[pl.ds(0, n - 1)], base_sems.at[0])


ANY = pl.BlockSpec(memory_space=pl.ANY)
VMEM = pl.BlockSpec(memory_space=pltpu.VMEM)
SMEM = pl.BlockSpec(memory_space=pltpu.SMEM)


def like(x):
    return jax.ShapeDtypeStruct(x.shape, x.dtype)


def exchange_counts(n, counts):
    lanes = min(counts.size, 128)
    shape = (counts.size // lanes, lanes)
    mine = counts.reshape(shape)
    peak = pl.pallas_call(
        functools.partial(counts_kernel, n),
        out_shape=like(mine),
        in_specs=[VMEM],
        out_specs=VMEM,
        scratch_shapes=[pltpu.VMEM((n,) + shape, jnp.int32)] + [pltpu.SemaphoreType.DMA] * 3,
        compiler_params=pltpu.CompilerParams(has_side_effects=True),
        name='counts',
    )(mine)
    return peak.reshape(counts.shape)


def dispatch_rows(n, source, rows, hot_rows, slices):
    sems = pltpu.SemaphoreType.DMA((3,))
    return pl.pallas_call(
        functools.partial(dispatch_kernel, n, HOT),
        out_shape=(like(rows), like(hot_rows), like(slices)),
        in_specs=[SMEM, ANY, ANY, ANY],
        out_specs=(ANY, ANY, ANY),
        scratch_shapes=[
            pltpu.VMEM(slices.shape, BF16),
            pltpu.VMEM((HOT,) + slices.shape[1:], BF16),
            sems, sems, sems, sems,
        ],
        compiler_params=pltpu.CompilerParams(has_side_effects=True),
        name='dispatch',
    )(source, rows, hot_rows, slices)


def return_rows(n, rows, hot_rows):
    sems = pltpu.SemaphoreType.DMA((3,))
    return pl.pallas_call(
        functools.partial(return_kernel, n, HOT),
        out_shape=(like(rows), like(hot_rows)),
        in_specs=[ANY, ANY],
        out_specs=(ANY, ANY),
        scratch_shapes=[sems, sems],
        compiler_params=pltpu.CompilerParams(has_side_effects=True),
        name='collect',
    )(rows, hot_rows)


def solution(mesh):
    group_size = mesh.shape['ep']

    def wide_layer(x_loc, idx_loc, gate_loc, w_in, w_out, shared_val):
        tok_rows, top_k = idx_loc.shape
        num_experts = w_in.shape[0] * group_size
        slot_cap = min(tok_rows, LOAD_MULT * tok_rows * top_k // num_experts)
        combine, dispatch = slot_tables(idx_loc, gate_loc, num_experts, slot_cap)
        send_rows = jnp.einsum('tec,tm->ecm', dispatch, x_loc, preferred_element_type=F32).astype(BF16)
        recv_rows = lax.all_to_all(send_rows, 'ep', 0, 1, tiled=True)
        hidden = gelu(jnp.einsum('erm,emf->erf', recv_rows, w_in, preferred_element_type=F32)).astype(BF16)
        expert_out = jnp.einsum('erf,efm->erm', hidden, w_out, preferred_element_type=F32).astype(BF16)
        back_rows = lax.all_to_all(expert_out, 'ep', 1, 0, tiled=True)
        routed = jnp.einsum('tec,ecm->tm', combine, back_rows, preferred_element_type=F32)
        return (routed + shared_val).astype(BF16)

    def local_layer(x_loc, idx_loc, gate_loc, w_in, w_out, shared_in, shared_out):
        tok_rows, top_k = idx_loc.shape
        d_model = x_loc.shape[1]
        ff_dim = w_in.shape[2]
        per_dev = w_in.shape[0]
        per_chip = per_dev * CORES
        num_experts = per_dev * group_size
        slot_cap = min(tok_rows, LOAD_MULT * tok_rows * top_k // num_experts)
        base_cap = min(BASE_CAP, slot_cap)
        over_cap = slot_cap - base_cap
        me = lax.axis_index('ep')
        chip, core = me // CORES, me % CORES

        partner = [(i, i ^ 1) for i in range(group_size)]
        other_in = lax.ppermute(w_in, 'ep', partner)
        other_out = lax.ppermute(w_out, 'ep', partner)

        expert_ids = jnp.arange(num_experts, dtype=jnp.int32)
        pick = idx_loc[:, :, None] == expert_ids
        picked = jnp.any(pick, axis=1)
        gate_rows = gate_loc.astype(BF16).astype(F32)
        gates = jnp.sum(jnp.where(pick, gate_rows[:, :, None], 0.0), axis=1).astype(BF16)
        ones = picked.astype(BF16)
        before = (jnp.arange(tok_rows)[:, None] > jnp.arange(tok_rows)[None, :]).astype(BF16)
        rank = jnp.dot(before, ones, preferred_element_type=F32)
        slot = jnp.where(picked, rank, -1.0).astype(BF16)

        counts = jnp.sum(picked.astype(jnp.int32), axis=0)
        peak = exchange_counts(group_size, counts)
        over = (peak > base_cap).astype(jnp.int32)
        over_rank = jnp.cumsum(over) - 1
        by_chip = over.reshape(group_size // CORES, per_chip)
        chip_rank = jnp.minimum(jnp.cumsum(by_chip, axis=1) - 1, CORES - 1).reshape(num_experts)
        fits = (jnp.sum(over) <= HOT) & (jnp.max(jnp.sum(by_chip, axis=1)) <= CORES)
        hot_sel = (over[:, None] > 0) & (over_rank[:, None] == jnp.arange(HOT, dtype=jnp.int32))
        holder = expert_ids // per_chip * CORES + chip_rank
        source = jnp.sum(jnp.where(hot_sel, holder[:, None], 0), axis=0)
        hot_sel = hot_sel.astype(BF16)

        local_over = lax.dynamic_slice(over, (chip * per_chip,), (per_chip,))
        local_rank = lax.dynamic_slice(chip_rank, (chip * per_chip,), (per_chip,))
        offered = (local_over > 0) & (local_rank == core)
        which = jnp.sum(jnp.where(offered, jnp.arange(per_chip, dtype=jnp.int32), 0))
        is_mine = which // per_dev == core
        which = which % per_dev

        def pick_weight(own, other):
            own = lax.dynamic_index_in_dim(own, which, 0, keepdims=False)
            other = lax.dynamic_index_in_dim(other, which, 0, keepdims=False)
            return jnp.where(is_mine, own, other)

        packed = jnp.concatenate([pick_weight(w_in, other_in).reshape(ff_dim, d_model), pick_weight(w_out, other_out)])
        slices = packed.reshape(group_size, 2 * ff_dim // group_size, d_model)

        base_rows = num_experts * base_cap
        owner = jnp.arange(base_rows, dtype=jnp.int32) // base_cap
        place = (jnp.arange(base_rows, dtype=jnp.int32) % base_cap).astype(F32)
        repeat = (expert_ids[:, None] == owner[None, :]).astype(BF16)
        slot_of = jnp.dot(slot, repeat, preferred_element_type=F32)
        gate_of = jnp.dot(gates, repeat, preferred_element_type=F32)
        base_unit = (slot_of == place).astype(BF16)
        base_gate = jnp.where(slot_of == place, gate_of, 0.0).astype(BF16)

        hot_count = HOT * over_cap
        hot_owner = jnp.arange(hot_count, dtype=jnp.int32) // over_cap
        hot_place = (jnp.arange(hot_count, dtype=jnp.int32) % over_cap + base_cap).astype(F32)
        hot_repeat = (jnp.arange(HOT, dtype=jnp.int32)[:, None] == hot_owner[None, :]).astype(BF16)
        hot_map = jnp.dot(hot_sel, hot_repeat, preferred_element_type=F32).astype(BF16)
        hot_slot_of = jnp.dot(slot, hot_map, preferred_element_type=F32)
        hot_gate_of = jnp.dot(gates, hot_map, preferred_element_type=F32)
        hot_unit = (hot_slot_of == hot_place).astype(BF16)
        hot_gate = jnp.where(hot_slot_of == hot_place, hot_gate_of, 0.0).astype(BF16)

        send = jnp.einsum('tr,tm->rm', base_unit, x_loc, preferred_element_type=F32).astype(BF16)
        hot_send = jnp.einsum('tr,tm->rm', hot_unit, x_loc, preferred_element_type=F32).astype(BF16)
        recv, hot_recv, team_w = dispatch_rows(
            group_size, source,
            send.reshape(group_size, per_dev * base_cap, d_model), hot_send.reshape(HOT, over_cap, d_model), slices,
        )
        team_w = team_w.reshape(2 * ff_dim, d_model)
        hot_in, hot_out = team_w[:ff_dim].reshape(d_model, ff_dim), team_w[ff_dim:]

        def ffn(rows, first, second):
            hidden = gelu(jnp.dot(rows, first, preferred_element_type=F32)).astype(BF16)
            return jnp.dot(hidden, second, preferred_element_type=F32)

        span = 2 * TILE
        first = ffn(recv[:, :span].reshape(group_size * span, d_model), w_in[0], w_out[0]).astype(BF16)
        second = ffn(recv[:, TILE:].reshape(group_size * span, d_model), w_in[1], w_out[1]).astype(BF16)
        first = first.reshape(group_size, span, d_model)
        second = second.reshape(group_size, span, d_model)
        middle = jnp.where(jnp.arange(TILE)[None, :, None] < base_cap - TILE, first[:, TILE:], second[:, :TILE])
        done = jnp.concatenate([first[:, :TILE], middle, second[:, TILE:]], axis=1)
        hot_done = ffn(hot_recv.reshape(hot_count, d_model), hot_in, hot_out).astype(BF16)

        back, hot_back = return_rows(group_size, done, hot_done.reshape(HOT, over_cap, d_model))
        back = back.reshape(base_rows, d_model)
        hot_back = hot_back.reshape(hot_count, d_model)

        shared_val = ffn(x_loc, shared_in, shared_out)
        routed = jnp.dot(base_gate, back, preferred_element_type=F32) + jnp.dot(hot_gate, hot_back, preferred_element_type=F32)
        tight = (routed + shared_val).astype(BF16)
        return lax.cond(
            fits,
            lambda *_: tight,
            lambda *args: wide_layer(*args),
            x_loc, idx_loc, gate_loc, w_in, w_out, shared_val,
        )

    tok_spec = P(('dp', 'ep'), None)
    expert_spec = P('ep', None, None)
    whole_spec = P(None, None)
    return jax.shard_map(local_layer, mesh=mesh, in_specs=(tok_spec, tok_spec, tok_spec, expert_spec, expert_spec, whole_spec, whole_spec), out_specs=tok_spec, check_vma=False)
```
